768 devices in a mesh: dom: 96 (over y_hi, z, core), sub: 8 (over x, y_lo).
Axes of the slice: x: 4, y: 8 (y_hi: 4, y_lo: 2; y = y_hi * 2 + y_lo), z: 12, core: 2. Of those that a mesh axis runs over, the one named last changes fastest.
Arguments:
- state: float32 [9, 10, 196608], P(None, None, ('dom', 'sub')), may hold values from -6 to 6
- geometry: float32 [3, 3, 196608], P(None, None, ('dom', 'sub')), may hold values from -4 to 4
- face_scale: float32 [4, 196608], P(None, ('dom', 'sub')), may hold values from 0.2 to 1
- material: int32 [196608], P(('dom', 'sub')), may hold values from 0 to 2
- cluster: int32 [196608], P(('dom', 'sub')), may hold values from 0 to 1, as said below
- neighbours: int32 [4, 196608], P(None, ('dom', 'sub')), may hold values from 0 to 1023, as said below
- orientation: int32 [4, 196608], P(None, ('dom', 'sub')), may hold values from 0 to 11
- stiffness: float32 [3, 10, 10], replicated, may hold values from -2 to 2
- jacobians: float32 [3, 3, 9, 9], replicated, may hold values from -2 to 2
- flux_local: float32 [4, 10, 10], replicated, may hold values from -2 to 2
- flux_neigh: float32 [12, 10, 10], replicated, may hold values from -2 to 2
- flux_plus: float32 [3, 9, 9], replicated, may hold values from -2 to 2
- flux_minus: float32 [3, 9, 9], replicated, may hold values from -2 to 2
Outputs:
- final_state: float32 [9, 10, 196608], P(None, None, ('dom', 'sub'))
The draws below stay inside these ranges and needn't reach their ends.
Inputs may be any that keep to these rules, and one draw needn't show every extreme that they name: Face neighbours are numbered in the table of the face's own partition, as the first step says. `cluster`: 0 marks a fine tetrahedron, 1 a coarse one.
All inputs are finite; a program needn't handle non-finite values.
Results may differ from the reference program's by a relative error of at most 0.0003.
Values sent between devices are 32-bit elements; how exact they have to be, the bound alone decides.
No kernel may reach another device: no remote copies, remote signals or barrier semaphores. Data moves between devices by JAX's collectives and lax.ppermute only.
A program may use at most 64 MiB of HBM per device.

```python
import math
import jax
import jax.numpy as jnp
from jax import lax

QUANT = 9
BASIS = 10
ELEM_DEV = 256
COPY_DEV = 128
SUB_COPY = 64
MACRO = 1
ELEMENTS = 196608
N_DOM = 96
N_SUB = 8


def draw_cluster(key, part):
    first_key = jax.random.fold_in(key, 11)
    second_key = jax.random.fold_in(key, 12)
    percent = jax.random.randint(first_key, (N_DOM * N_SUB,), 10, 91)
    rolled = jax.random.randint(second_key, (ELEMENTS,), 0, 100)
    owner = jnp.arange(ELEMENTS, dtype=jnp.int32) // ELEM_DEV
    return jnp.where(rolled < percent[owner], 0, 1).astype(jnp.int32)


def draw_neighbours(key, part):
    local_key = jax.random.fold_in(key, 21)
    sub_key = jax.random.fold_in(key, 22)
    side_key = jax.random.fold_in(key, 23)
    local_pick = jax.random.randint(local_key, (4, ELEMENTS), 0, ELEM_DEV)
    sub_pick = jax.random.randint(sub_key, (ELEMENTS,), 0, N_SUB * SUB_COPY)
    side_pick = jax.random.randint(side_key, (2, ELEMENTS), 0, COPY_DEV)
    local = jnp.arange(ELEMENTS, dtype=jnp.int32) % ELEM_DEV
    left_start = ELEM_DEV + N_SUB * SUB_COPY
    right_start = left_start + COPY_DEV
    face_zero = jnp.where(local < SUB_COPY, ELEM_DEV + sub_pick, local_pick[0])
    face_one = jnp.where(local >= ELEM_DEV - COPY_DEV, right_start + side_pick[0], local_pick[1])
    face_two = jnp.where(local < COPY_DEV, left_start + side_pick[1], local_pick[2])
    return jnp.stack([face_zero, face_one, face_two, local_pick[3]]).astype(jnp.int32)


def place_ends(values, key, smallest, top_value):
    place = [jax.random.randint(jax.random.fold_in(key, axis), (), 0, length) for axis, length in enumerate(values.shape)]
    longest = values.shape.index(max(values.shape))
    neighbour = place[:longest] + [(place[longest] + 1) % values.shape[longest]] + place[longest + 1:]
    return values.at[tuple(place)].set(smallest).at[tuple(neighbour)].set(top_value)


def steps_of(stream_key, extent, cuts, least, top_value):
    gain, own = 1.0, jax.random.fold_in(stream_key, 6)
    for dim, blocks in cuts:
        heights = jnp.exp(jax.random.uniform(jax.random.fold_in(own, dim), (blocks,), jnp.float32, least / len(cuts), top_value / len(cuts)))
        gain = gain * jnp.repeat(heights, extent[dim] // blocks).reshape([-1 if axis == dim else 1 for axis in range(len(extent))])
    return gain


def bell_draw(rng, dims, width, reach, shards=(), held_as=jnp.bfloat16):
    entries = width * jax.random.normal(rng, dims, jnp.float32)
    if shards:
        entries = entries * steps_of(rng, dims, shards, -0.22, 0.18)
    return jnp.clip(entries, -reach, reach).astype(held_as)


def setup_inputs(seed: int = 0) -> dict:
    seeds = jax.random.split(jax.random.key(seed), 14)
    state = bell_draw(seeds[0], (QUANT, BASIS, ELEMENTS), 1.0, 6.0, ((2, 768),), jnp.float32)
    geometry = bell_draw(seeds[1], (3, 3, ELEMENTS), 0.6, 4.0, ((2, 768),), jnp.float32)
    face_scale = jnp.clip(jnp.exp(math.log(1.0) - 1.609438 * jax.random.uniform(seeds[2], (4, ELEMENTS), jnp.float32) ** steps_of(seeds[2], (4, ELEMENTS), ((1, 768),), -0.2, 0.2)), 0.2, 1.0)
    material = place_ends(jax.random.randint(seeds[3], (ELEMENTS,), 0, 3), jax.random.fold_in(seeds[3], 1), 0, 2).astype(jnp.int32)
    cluster = draw_cluster(jax.random.fold_in(seeds[13], 71), 0)
    neighbours = draw_neighbours(jax.random.fold_in(seeds[13], 71), 0)
    orientation = place_ends(jax.random.randint(seeds[6], (4, ELEMENTS), 0, 12), jax.random.fold_in(seeds[6], 1), 0, 11).astype(jnp.int32)
    stiffness = bell_draw(seeds[7], (3, BASIS, BASIS), BASIS ** -0.5, 2.0, (), jnp.float32)
    jacobians = bell_draw(seeds[8], (3, 3, QUANT, QUANT), QUANT ** -0.5, 2.0, (), jnp.float32)
    flux_local = bell_draw(seeds[9], (4, BASIS, BASIS), BASIS ** -0.5, 2.0, (), jnp.float32)
    flux_neigh = bell_draw(seeds[10], (12, BASIS, BASIS), BASIS ** -0.5, 2.0, (), jnp.float32)
    flux_plus = bell_draw(seeds[11], (3, QUANT, QUANT), QUANT ** -0.5, 2.0, (), jnp.float32)
    flux_minus = bell_draw(seeds[12], (3, QUANT, QUANT), QUANT ** -0.5, 2.0, (), jnp.float32)
    return {"state": state, "geometry": geometry, "face_scale": face_scale, "material": material, "cluster": cluster, "neighbours": neighbours, "orientation": orientation, "stiffness": stiffness, "jacobians": jacobians, "flux_local": flux_local, "flux_neigh": flux_neigh, "flux_plus": flux_plus, "flux_minus": flux_minus}


step_length = 0.2


def per_element(matrix, values):
    total = matrix[:, 0][:, None, :] * values[0][None, :, :]
    for inner in range(1, matrix.shape[1]):
        total = total + matrix[:, inner][:, None, :] * values[inner][None, :, :]
    return total


def per_element_basis(matrix, values):
    total = matrix[None, :, 0, :] * values[:, 0][:, None, :]
    for inner in range(1, matrix.shape[1]):
        total = total + matrix[None, :, inner, :] * values[:, inner][:, None, :]
    return total


def apply_star(values, stiffness, geometry, element_jac, transpose):
    pattern = "ba,vbe->vae" if transpose else "ab,vbe->vae"
    mapped = [jnp.einsum(pattern, stiffness[direction], values, precision=lax.Precision.HIGHEST) for direction in range(3)]
    summed = jnp.zeros_like(values)
    for column in range(3):
        mixture = mapped[0] * geometry[0, column] + mapped[1] * geometry[1, column] + mapped[2] * geometry[2, column]
        summed = summed + per_element(element_jac[column], mixture)
    return summed


def predict(values, stiffness, geometry, element_jac, coarse, shifted):
    first = -apply_star(values, stiffness, geometry, element_jac, False)
    second = -apply_star(first, stiffness, geometry, element_jac, False)
    if shifted:
        values = values + coarse * (step_length * first + 0.5 * step_length ** 2 * second)
        first = first + coarse * (step_length * second)
    return step_length * values + (step_length ** 2 / 2) * first + (step_length ** 3 / 6) * second


def update(own, neighbour_parts, face_scale, stiffness, geometry, element_jac, element_plus, element_minus, face_neigh, flux_local):
    result = apply_star(own, stiffness, geometry, element_jac, True)
    plus = per_element(element_plus, own)
    for face in range(4):
        minus = per_element(element_minus, neighbour_parts[face])
        across = jnp.einsum("ab,vbe->vae", flux_local[face], plus, precision=lax.Precision.HIGHEST)
        across = across + per_element_basis(face_neigh[face], minus)
        result = result - face_scale[face] * across
    return result


def element_tables(material, orientation, jacobians, flux_plus, flux_minus, flux_neigh):
    medium_mask = (material[None, :] == jnp.arange(3, dtype=jnp.int32)[:, None]).astype(jnp.float32)
    element_jac = jnp.einsum("mcvw,me->cvwe", jacobians, medium_mask, precision=lax.Precision.HIGHEST)
    element_plus = jnp.einsum("mvw,me->vwe", flux_plus, medium_mask, precision=lax.Precision.HIGHEST)
    element_minus = jnp.einsum("mvw,me->vwe", flux_minus, medium_mask, precision=lax.Precision.HIGHEST)
    turns = jnp.arange(12, dtype=jnp.int32)[:, None]
    face_neigh = [jnp.einsum("tab,te->abe", flux_neigh, (orientation[face][None, :] == turns).astype(jnp.float32), precision=lax.Precision.HIGHEST) for face in range(4)]
    return element_jac, element_plus, element_minus, face_neigh


def global_index(neighbours):
    glob = jnp.arange(ELEMENTS, dtype=jnp.int32)
    owner = glob // ELEM_DEV
    dom_index = owner // N_SUB
    sub_index = owner % N_SUB
    sub_start = ELEM_DEV
    left_start = ELEM_DEV + N_SUB * SUB_COPY
    right_start = left_start + COPY_DEV
    local_glob = owner * ELEM_DEV + neighbours
    offset = neighbours - sub_start
    sub_glob = (dom_index * N_SUB + offset // SUB_COPY) * ELEM_DEV + offset % SUB_COPY
    left_glob = (jnp.mod(dom_index - 1, N_DOM) * N_SUB + sub_index) * ELEM_DEV + ELEM_DEV - COPY_DEV + (neighbours - left_start)
    right_glob = (jnp.mod(dom_index + 1, N_DOM) * N_SUB + sub_index) * ELEM_DEV + (neighbours - right_start)
    result = jnp.where(neighbours < sub_start, local_glob, sub_glob)
    result = jnp.where(neighbours >= left_start, left_glob, result)
    result = jnp.where(neighbours >= right_start, right_glob, result)
    return result.astype(jnp.int32)


def reference(state, geometry, face_scale, material, cluster, neighbours, orientation, stiffness, jacobians, flux_local, flux_neigh, flux_plus, flux_minus):
    element_jac, element_plus, element_minus, face_neigh = element_tables(material, orientation, jacobians, flux_plus, flux_minus, flux_neigh)
    coarse = cluster.astype(jnp.float32)
    finer = 1.0 - coarse
    indices = global_index(neighbours)

    def advance(integral):
        parts = [jnp.take(integral, indices[face], axis=2) for face in range(4)]
        return update(integral, parts, face_scale, stiffness, geometry, element_jac, element_plus, element_minus, face_neigh, flux_local)

    for outer_step in range(MACRO):
        first_change = advance(predict(state, stiffness, geometry, element_jac, coarse, False))
        middle = state + finer * first_change
        second_change = advance(predict(middle, stiffness, geometry, element_jac, coarse, True))
        state = middle + finer * second_change + coarse * (first_change + second_change)
    return state
```

```python
import jax
import jax.numpy as jnp
from jax import lax
from jax.experimental import pallas as pl
from jax.experimental.pallas import tpu as pltpu
from jax.sharding import PartitionSpec as P

V = 9
B = 10
E = 256
COPY = 128
SUBC = 64
ROWS = 96
DT = 0.2
EXACT = lax.Precision.HIGHEST
f32 = jnp.float32
bf16 = jnp.bfloat16


def row_of(w, b):
    return w * 8 + b if b < 8 else 72 + 2 * w + b - 8


def by_material(material, pick):
    first = jnp.broadcast_to(material == 0, (V, E))
    second = jnp.broadcast_to(material == 1, (V, E))
    column = [jnp.broadcast_to(pick(m), (V, E)) for m in range(3)]
    return jnp.where(first, column[0], jnp.where(second, column[1], column[2]))


def mapped(matrix, values, out_ref):
    wide = jnp.concatenate(values, axis=1)
    out_ref[...] = jnp.dot(matrix, wide, precision=EXACT, preferred_element_type=f32)


def block(ref, row, w):
    return ref[16 * row : 16 * row + B, w * E : (w + 1) * E]


def mixed(total, matrix_ref, index, value):
    for v in range(V):
        term = matrix_ref[index, v : v + 1, :] * value
        total[v] = term if total[v] is None else total[v] + term


def star(values, matrix, jac_ref, y_ref):
    mapped(matrix, values, y_ref)
    total = [None] * V
    for i in range(3):
        for w in range(V):
            mixed(total, jac_ref, i * V + w, block(y_ref, i, w))
    return total


def padded_stiffness(stiffness_ref, k_ref):
    k_ref[...] = jnp.zeros_like(k_ref)
    for i in range(3):
        k_ref[16 * i : 16 * i + B, :] = stiffness_ref[i]


def pack(values, p_ref, lower_ref, upper_ref, sub_ref):
    for v in range(V):
        p_ref[8 * v : 8 * v + 8, :] = values[v][:8]
        p_ref[72 + 2 * v : 74 + 2 * v, :] = values[v][8:]
    p_ref[90:ROWS, :] = jnp.zeros((ROWS - 90, E), f32)
    low = p_ref[:, :COPY]
    lower_ref[...] = low
    upper_ref[...] = p_ref[:, COPY:]
    lane = lax.broadcasted_iota(jnp.int32, (48, 128), 1)
    sub_ref[...] = jnp.where(lane < SUBC, low[:48], pltpu.roll(low[48:], SUBC, 1))


def first_kernel(
    state_ref, geo_ref, mat_ref, jac_ref, stiff_ref,
    ejac_ref, j_ref, p_ref, lower_ref, upper_ref, sub_ref, k_ref, y_ref,
):
    material = mat_ref[...]
    padded_stiffness(stiff_ref, k_ref)
    for w in range(V):
        parts = [
            by_material(material, lambda m: jac_ref[m, c, :, w : w + 1]) for c in range(3)
        ]
        for i in range(3):
            ejac_ref[i * V + w] = (
                geo_ref[i, 0:1, :] * parts[0]
                + geo_ref[i, 1:2, :] * parts[1]
                + geo_ref[i, 2:3, :] * parts[2]
            )
    values = [state_ref[v] for v in range(V)]
    matrix = k_ref[...]
    one = star(values, matrix, ejac_ref, y_ref)
    two = star(one, matrix, ejac_ref, y_ref)
    out = []
    for v in range(V):
        integral = DT * state_ref[v] - DT**2 / 2 * one[v] + DT**3 / 6 * two[v]
        j_ref[v] = integral
        out.append(integral)
    pack(out, p_ref, lower_ref, upper_ref, sub_ref)


def split(values):
    high = values.astype(bf16)
    low = (values - high.astype(f32)).astype(bf16)
    return jnp.concatenate([high, low], axis=0)


def one_hot(index, start, count):
    places = lax.broadcasted_iota(jnp.int32, (count, E), 0) + start
    return jnp.where(places == index, 1.0, 0.0).astype(bf16)


def gathered(pieces, picks, n_ref):
    for face in range(4):
        both = jnp.dot(pieces, picks(face), preferred_element_type=f32)
        n_ref[:, face * E : (face + 1) * E] = both[:ROWS] + both[ROWS:]


def neighbour_flux(n_ref, turn_ref, minus_ref, total):
    for face in range(4):
        lanes = slice(face * E, (face + 1) * E)
        if face == 0:
            across = [None] * V
        for b in range(B):
            turn = turn_ref[face * B + b]
            for w in range(V):
                row = row_of(w, b)
                term = turn * n_ref[row : row + 1, lanes]
                across[w] = term if across[w] is None else across[w] + term
    for w in range(V):
        mixed(total, minus_ref, w, across[w])
    return total


def local_part(j_ref, p_ref, matrix, scale_ref, ejac_ref, plus_ref, minus_ref, turn_ref,
               picks, y_ref, n_ref, out_ref):
    mapped(matrix, [j_ref[v] for v in range(V)], y_ref)
    gathered(split(p_ref[...]), picks, n_ref)
    total = [None] * V
    for i in range(3):
        for w in range(V):
            mixed(total, ejac_ref, i * V + w, block(y_ref, i, w))
    for v in range(V):
        out_ref[v] = total[v]
    total = [None] * V
    for w in range(V):
        own = scale_ref[0:1, :] * block(y_ref, 3, w)
        for face in range(1, 4):
            own = own + scale_ref[face : face + 1, :] * block(y_ref, 3 + face, w)
        mixed(total, plus_ref, w, own)
    for v in range(V):
        out_ref[v] = out_ref[v] - total[v]
    total = neighbour_flux(n_ref, turn_ref, minus_ref, [None] * V)
    for v in range(V):
        out_ref[v] = out_ref[v] - total[v]


def local_kernel_one(
    j_ref, p_ref, ejac_ref, matrix_ref, mat_ref, near_ref, orient_ref, scale_ref,
    fplus_ref, fminus_ref, fneigh_ref,
    out_ref, plus_ref, minus_ref, turn_ref, here_ref, there_ref, y_ref, n_ref,
):
    material = mat_ref[...]
    for w in range(V):
        plus_ref[w] = by_material(material, lambda m: fplus_ref[m, :, w : w + 1])
        minus_ref[w] = by_material(material, lambda m: fminus_ref[m, :, w : w + 1])
    for face in range(4):
        index = near_ref[face : face + 1, :]
        here_ref[face] = one_hot(index, 0, E)
        there_ref[face] = one_hot(index, E, 768)
        way = orient_ref[face : face + 1, :]
        scale = scale_ref[face : face + 1, :]
        masks = [jnp.broadcast_to(way == t, (B, E)) for t in range(11)]
        for b in range(B):
            chosen = jnp.broadcast_to(fneigh_ref[11, :, b : b + 1], (B, E))
            for t in range(11):
                column = jnp.broadcast_to(fneigh_ref[t, :, b : b + 1], (B, E))
                chosen = jnp.where(masks[t], column, chosen)
            turn_ref[face * B + b] = chosen * scale
    local_part(j_ref, p_ref, matrix_ref[...], scale_ref, ejac_ref, plus_ref, minus_ref,
               turn_ref, lambda face: here_ref[face], y_ref, n_ref, out_ref)


def local_kernel_two(
    j_ref, p_ref, ejac_ref, matrix_ref, scale_ref, plus_ref, minus_ref, turn_ref, here_ref,
    out_ref, y_ref, n_ref,
):
    local_part(j_ref, p_ref, matrix_ref[...], scale_ref, ejac_ref, plus_ref, minus_ref,
               turn_ref, lambda face: here_ref[face], y_ref, n_ref, out_ref)


def remote_flux(group_ref, left_ref, right_ref, there_ref, turn_ref, minus_ref, n_ref):
    lane = lax.broadcasted_iota(jnp.int32, (48, 128), 1)
    table = []
    for pair in range(4):
        one = group_ref[2 * pair]
        two = group_ref[2 * pair + 1]
        top = jnp.where(lane < SUBC, one, pltpu.roll(two, SUBC, 1))
        bottom = jnp.where(lane < SUBC, pltpu.roll(one, SUBC, 1), two)
        table.append(jnp.concatenate([top, bottom], axis=0))
    table += [left_ref[...], right_ref[...]]
    pieces = split(jnp.concatenate(table, axis=1))
    gathered(pieces, lambda face: there_ref[face], n_ref)
    return neighbour_flux(n_ref, turn_ref, minus_ref, [None] * V)


def middle_kernel(
    state_ref, local_ref, group_ref, left_ref, right_ref, there_ref, turn_ref, minus_ref,
    ejac_ref, stiff_ref, cluster_ref,
    base_ref, j_ref, p_ref, lower_ref, upper_ref, sub_ref, n_ref, k_ref, y_ref, m_ref,
):
    flux = remote_flux(group_ref, left_ref, right_ref, there_ref, turn_ref, minus_ref, n_ref)
    coarse = cluster_ref[...].astype(f32)
    fine = 1.0 - coarse
    for v in range(V):
        change = local_ref[v] - flux[v]
        base_ref[v] = state_ref[v] + change
        m_ref[v] = state_ref[v] + fine * change
    padded_stiffness(stiff_ref, k_ref)
    matrix = k_ref[...]
    one = star([m_ref[v] for v in range(V)], matrix, ejac_ref, y_ref)
    two = star(one, matrix, ejac_ref, y_ref)
    weight_one = DT**2 / 2 + DT**2 * coarse
    weight_two = DT**3 / 6 + DT**3 * coarse
    out = []
    for v in range(V):
        integral = DT * m_ref[v] - weight_one * one[v] + weight_two * two[v]
        j_ref[v] = integral
        out.append(integral)
    pack(out, p_ref, lower_ref, upper_ref, sub_ref)


def last_kernel(
    base_ref, local_ref, group_ref, left_ref, right_ref, there_ref, turn_ref, minus_ref,
    out_ref, n_ref,
):
    flux = remote_flux(group_ref, left_ref, right_ref, there_ref, turn_ref, minus_ref, n_ref)
    for v in range(V):
        out_ref[v] = base_ref[v] + (local_ref[v] - flux[v])


def arr(*shape, dtype=f32):
    return jax.ShapeDtypeStruct(shape, dtype)


def call(kernel, outs, scratch, flops, name):
    return pl.pallas_call(
        kernel,
        out_shape=outs,
        scratch_shapes=[pltpu.VMEM(s, f32) for s in scratch],
        compiler_params=pltpu.CompilerParams(vmem_limit_bytes=24 << 20),
        cost_estimate=pl.CostEstimate(flops=flops, bytes_accessed=1 << 20, transcendentals=0),
        name=name,
    )


def sent(value, axis, shift):
    size = lax.axis_size(axis)
    return lax.ppermute(value, axis, [((i - shift) % size, i) for i in range(size)])


def exchange(lower, upper, sub):
    left = sent(upper, "dom", 1)
    right = sent(lower, "dom", -1)
    group = lax.all_to_all(
        jnp.broadcast_to(sub[None], (8, *sub.shape)), "sub", 0, 0, tiled=True
    )
    return group, left, right


def shards(state, geometry, face_scale, material, cluster, neighbours, orientation,
           stiffness, jacobians, flux_local, flux_neigh, flux_plus, flux_minus):
    material = material.reshape(1, E)
    cluster = cluster.reshape(1, E)
    cube = arr(V, B, E)
    packed = [arr(ROWS, E), arr(ROWS, COPY), arr(ROWS, COPY), arr(48, 128)]
    wide = (112, V * E)
    narrow = (48, V * E)
    picked = (ROWS, 4 * E)

    ejac, j0, p0, lower, upper, sub = call(
        first_kernel, [arr(27, V, E), cube, *packed], [(48, B), narrow], 1 << 28, "first"
    )(state, geometry, material, jacobians, stiffness)
    remote0 = exchange(lower, upper, sub)
    matrix = jnp.concatenate([jnp.swapaxes(stiffness, 1, 2), flux_local], axis=0)
    matrix = jnp.pad(matrix, ((0, 0), (0, 6), (0, 0))).reshape(112, B)
    local0, plus, minus, turn, here, there = call(
        local_kernel_one,
        [cube, arr(V, V, E), arr(V, V, E), arr(4 * B, B, E),
         arr(4, E, E, dtype=bf16), arr(4, 768, E, dtype=bf16)],
        [wide, picked], 1 << 33, "local_one",
    )(j0, p0, ejac, matrix, material, neighbours, orientation, face_scale,
      flux_plus, flux_minus, flux_neigh)
    base, j1, p1, lower, upper, sub = call(
        middle_kernel, [cube, cube, *packed],
        [picked, (48, B), narrow, (V, B, E)], 1 << 28, "middle",
    )(state, local0, *remote0, there, turn, minus, ejac, stiffness, cluster)
    remote1 = exchange(lower, upper, sub)
    local1 = call(local_kernel_two, cube, [wide, picked], 1 << 33, "local_two")(
        j1, p1, ejac, matrix, face_scale, plus, minus, turn, here
    )
    return call(last_kernel, cube, [picked], 1 << 28, "last")(
        base, local1, *remote1, there, turn, minus
    )


def solution(mesh):
    whole = ("dom", "sub")
    placed = (
        P(None, None, whole), P(None, None, whole), P(None, whole), P(whole), P(whole),
        P(None, whole), P(None, whole), P(), P(), P(), P(), P(), P(),
    )
    return jax.shard_map(
        shards, mesh=mesh, in_specs=placed, out_specs=P(None, None, whole), check_vma=False
    )
```

```python
import jax
import jax.numpy as jnp
from jax import lax
from jax.experimental import pallas as pl
from jax.experimental.pallas import tpu as pltpu
from jax.sharding import PartitionSpec as P

V = 9
B = 10
E = 256
COPY = 128
SUBC = 64
ROWS = 96
DT = 0.2
EXACT = lax.Precision.HIGH
f32 = jnp.float32
bf16 = jnp.bfloat16


def row_of(w, b):
    return w * 8 + b if b < 8 else 72 + 2 * w + b - 8


def by_material(material, pick):
    first = jnp.broadcast_to(material == 0, (V, E))
    second = jnp.broadcast_to(material == 1, (V, E))
    column = [jnp.broadcast_to(pick(m), (V, E)) for m in range(3)]
    return jnp.where(first, column[0], jnp.where(second, column[1], column[2]))


def mapped(matrix, values, out_ref):
    wide = jnp.concatenate(values, axis=1)
    out_ref[...] = jnp.dot(matrix, wide, precision=EXACT, preferred_element_type=f32)


def block(ref, row, w):
    return ref[16 * row : 16 * row + B, w * E : (w + 1) * E]


def mixed(total, matrix_ref, index, value):
    for v in range(V):
        row = index * V + v
        term = matrix_ref[row : row + 1, :] * value
        total[v] = term if total[v] is None else total[v] + term


def star(values, matrix, jac_ref, y_ref):
    mapped(matrix, values, y_ref)
    total = [None] * V
    for i in range(3):
        for w in range(V):
            mixed(total, jac_ref, i * V + w, block(y_ref, i, w))
    return total


def padded_stiffness(stiffness_ref, k_ref):
    k_ref[...] = jnp.zeros_like(k_ref)
    for a in range(B):
        for i in range(3):
            k_ref[16 * i + a : 16 * i + a + 1, :] = stiffness_ref[a, i : i + 1, :]


def by_matrix(rows_ref, out_ref):
    for a in range(rows_ref.shape[0]):
        for t in range(rows_ref.shape[1]):
            out_ref[t, a : a + 1, :] = rows_ref[a, t : t + 1, :]


def is_even():
    return lax.rem(lax.axis_index("dom"), 2) == 0


def pack(values, p_ref, outer_ref, inner_ref, sub_ref):
    for v in range(V):
        p_ref[8 * v : 8 * v + 8, :] = values[v][:8]
        p_ref[72 + 2 * v : 74 + 2 * v, :] = values[v][8:]
    p_ref[90:ROWS, :] = jnp.zeros((ROWS - 90, E), f32)
    low = p_ref[:, :COPY]
    high = p_ref[:, COPY:]
    even = is_even()
    outer_ref[...] = jnp.where(even, low, high)
    inner_ref[...] = jnp.where(even, high, low)
    lane = lax.broadcasted_iota(jnp.int32, (48, 128), 1)
    sub = jnp.where(lane < SUBC, low[:48], pltpu.roll(low[48:], SUBC, 1))
    for k in range(8):
        sub_ref[k] = sub


def first_kernel(wait, ins, outs, scratch):
    jac_ref, mat_ref, geo_ref, stiff_ref, state_ref = ins
    ejac_ref, p_ref, outer_ref, inner_ref, sub_ref = outs
    k_ref, y_ref, matrix_ref = scratch
    wait(0)
    for m in range(3):
        for v in range(V):
            for c in range(3):
                matrix_ref[m * 3 + c, v : v + 1, :] = jac_ref[m, v, c : c + 1, :]
    wait(1, 2)
    material = mat_ref[...]
    for w in range(V):
        parts = [
            by_material(material, lambda m: matrix_ref[m * 3 + c, :, w : w + 1])
            for c in range(3)
        ]
        for i in range(3):
            row = (i * V + w) * V
            ejac_ref[row : row + V, :] = (
                geo_ref[i, 0:1, :] * parts[0]
                + geo_ref[i, 1:2, :] * parts[1]
                + geo_ref[i, 2:3, :] * parts[2]
            )
    wait(3, 4)
    padded_stiffness(stiff_ref, k_ref)
    values = [state_ref[v] for v in range(V)]
    matrix = k_ref[...]
    one = star(values, matrix, ejac_ref, y_ref)
    two = star(one, matrix, ejac_ref, y_ref)
    out = [
        DT * state_ref[v] - DT**2 / 2 * one[v] + DT**3 / 6 * two[v] for v in range(V)
    ]
    pack(out, p_ref, outer_ref, inner_ref, sub_ref)


def split(values):
    high = values.astype(bf16)
    low = (values - high.astype(f32)).astype(bf16)
    return jnp.concatenate([high, low], axis=0)


def one_hot(index, start, count):
    places = lax.broadcasted_iota(jnp.int32, (count, E), 0) + start
    return jnp.where(places == index, 1.0, 0.0).astype(bf16)


def gathered(pieces, picks, n_ref):
    for face in range(4):
        both = jnp.dot(pieces, picks(face), preferred_element_type=f32)
        n_ref[:, face * E : (face + 1) * E] = both[:ROWS] + both[ROWS:]


def neighbour_flux(n_ref, turn_ref, minus_ref, total):
    for face in range(4):
        lanes = slice(face * E, (face + 1) * E)
        if face == 0:
            across = [None] * V
        for b in range(B):
            turn = turn_ref[face * B + b]
            for w in range(V):
                row = row_of(w, b)
                term = turn * n_ref[row : row + 1, lanes]
                across[w] = term if across[w] is None else across[w] + term
    for w in range(V):
        mixed(total, minus_ref, w, across[w])
    return total


def unpacked(p_ref, v):
    tail = 72 + 2 * v
    return jnp.concatenate([p_ref[8 * v : 8 * v + 8, :], p_ref[tail : tail + 2, :]], axis=0)


def local_part(p_ref, matrix_ref, near_ref, scale_ref, ejac_ref, plus_ref, minus_ref,
               turn_ref, y_ref, n_ref, out_ref):
    picks = lambda face: one_hot(near_ref[face : face + 1, :], 0, E)
    mapped(matrix_ref[...], [unpacked(p_ref, v) for v in range(V)], y_ref)
    gathered(split(p_ref[...]), picks, n_ref)
    total = [None] * V
    for i in range(3):
        for w in range(V):
            mixed(total, ejac_ref, i * V + w, block(y_ref, i, w))
    for v in range(V):
        out_ref[v] = total[v]
    total = [None] * V
    for w in range(V):
        own = scale_ref[0:1, :] * block(y_ref, 3, w)
        for face in range(1, 4):
            own = own + scale_ref[face : face + 1, :] * block(y_ref, 3 + face, w)
        mixed(total, plus_ref, w, own)
    for v in range(V):
        out_ref[v] = out_ref[v] - total[v]
    total = neighbour_flux(n_ref, turn_ref, minus_ref, [None] * V)
    for v in range(V):
        out_ref[v] = out_ref[v] - total[v]


def local_kernel_one(wait, ins, outs, scratch):
    (fneigh_ref, orient_ref, scale_ref, fplus_ref, fminus_ref, mat_ref, stiff_ref,
     flocal_ref, near_ref, p_ref, ejac_ref) = ins
    out_ref, plus_ref, minus_ref, turn_ref, matrix_ref = outs
    y_ref, n_ref, rows_plus, rows_minus, rows_neigh, k_ref = scratch
    wait(0, 1, 2)
    by_matrix(fneigh_ref, rows_neigh)
    for face in range(4):
        way = orient_ref[face : face + 1, :]
        scale = scale_ref[face : face + 1, :]
        masks = [jnp.broadcast_to(way == t, (B, E)) for t in range(11)]
        for b in range(B):
            chosen = jnp.broadcast_to(rows_neigh[11, :, b : b + 1], (B, E))
            for t in range(11):
                column = jnp.broadcast_to(rows_neigh[t, :, b : b + 1], (B, E))
                chosen = jnp.where(masks[t], column, chosen)
            turn_ref[face * B + b] = chosen * scale
    wait(3, 4, 5)
    material = mat_ref[...]
    by_matrix(fplus_ref, rows_plus)
    by_matrix(fminus_ref, rows_minus)
    for w in range(V):
        rows = slice(w * V, w * V + V)
        plus_ref[rows, :] = by_material(material, lambda m: rows_plus[m, :, w : w + 1])
        minus_ref[rows, :] = by_material(material, lambda m: rows_minus[m, :, w : w + 1])
    wait(6, 7)
    padded_stiffness(stiff_ref, k_ref)
    matrix_ref[...] = jnp.zeros_like(matrix_ref)
    for i in range(3):
        matrix_ref[16 * i : 16 * i + B, :] = k_ref[16 * i : 16 * i + B, :].T
    for a in range(B):
        for face in range(4):
            row = 48 + 16 * face + a
            matrix_ref[row : row + 1, :] = flocal_ref[a, face : face + 1, :]
    wait(8, 9, 10)
    local_part(p_ref, matrix_ref, near_ref, scale_ref, ejac_ref, plus_ref, minus_ref,
               turn_ref, y_ref, n_ref, out_ref)


def local_kernel_two(wait, ins, outs, scratch):
    p_ref, matrix_ref, near_ref, ejac_ref, scale_ref, plus_ref, turn_ref, minus_ref = ins
    wait(*range(8))
    local_part(p_ref, matrix_ref, near_ref, scale_ref, ejac_ref, plus_ref, minus_ref,
               turn_ref, *scratch, *outs)


def remote_flux(wait, ins, n_ref):
    near_ref, outer_ref, inner_ref, group_ref, turn_ref, minus_ref = ins
    even = is_even()

    def picks(face):
        index = near_ref[face : face + 1, :]
        swapped = jnp.where(index >= 768, index ^ 128, index)
        return one_hot(jnp.where(even, index, swapped), E, 768)

    wait(0, 1, 2, 3)
    lane = lax.broadcasted_iota(jnp.int32, (48, 128), 1)
    table = []
    for pair in range(4):
        one = group_ref[2 * pair]
        two = group_ref[2 * pair + 1]
        top = jnp.where(lane < SUBC, one, pltpu.roll(two, SUBC, 1))
        bottom = jnp.where(lane < SUBC, pltpu.roll(one, SUBC, 1), two)
        table.append(jnp.concatenate([top, bottom], axis=0))
    table += [outer_ref[...], inner_ref[...]]
    gathered(split(jnp.concatenate(table, axis=1)), picks, n_ref)
    wait(4, 5)
    return neighbour_flux(n_ref, turn_ref, minus_ref, [None] * V)


def middle_kernel(wait, ins, outs, scratch):
    state_ref, local_ref, cluster_ref, ejac_ref, stiff_ref = ins[6:]
    base_ref, p_ref, outer_ref, inner_ref, sub_ref = outs
    n_ref, k_ref, y_ref, m_ref = scratch
    flux = remote_flux(wait, ins[:6], n_ref)
    wait(6, 7, 8)
    coarse = cluster_ref[...].astype(f32)
    fine = 1.0 - coarse
    for v in range(V):
        change = local_ref[v] - flux[v]
        base_ref[v] = state_ref[v] + change
        m_ref[v] = state_ref[v] + fine * change
    wait(9, 10)
    padded_stiffness(stiff_ref, k_ref)
    matrix = k_ref[...]
    one = star([m_ref[v] for v in range(V)], matrix, ejac_ref, y_ref)
    two = star(one, matrix, ejac_ref, y_ref)
    weight_one = DT**2 / 2 + DT**2 * coarse
    weight_two = DT**3 / 6 + DT**3 * coarse
    out = [
        DT * m_ref[v] - weight_one * one[v] + weight_two * two[v] for v in range(V)
    ]
    pack(out, p_ref, outer_ref, inner_ref, sub_ref)


def last_kernel(wait, ins, outs, scratch):
    base_ref, local_ref = ins[6:]
    flux = remote_flux(wait, ins[:6], *scratch)
    wait(6, 7)
    for v in range(V):
        outs[0][v] = base_ref[v] + (local_ref[v] - flux[v])


def arr(*shape, dtype=f32):
    return jax.ShapeDtypeStruct(shape, dtype)


def call(kernel, outs, scratch, flops, *operands):
    count = len(operands)

    def body(*refs):
        given, rest = refs[:count], refs[count:]
        results, rest = rest[: len(outs)], rest[len(outs) :]
        held, rest = rest[:count], rest[count:]
        copies = [
            pltpu.make_async_copy(given[i], held[i], rest[-1].at[i]) for i in range(count)
        ]
        for copy in copies:
            copy.start()

        def wait(*which):
            for i in which:
                copies[i].wait()

        kernel(wait, held, results, rest[:-1])

    return pl.pallas_call(
        body,
        out_shape=outs,
        in_specs=[pl.BlockSpec(memory_space=pltpu.HBM)] * count,
        scratch_shapes=[pltpu.VMEM(x.shape, x.dtype) for x in operands]
        + [pltpu.VMEM(shape, f32) for shape in scratch]
        + [pltpu.SemaphoreType.DMA((count,))],
        compiler_params=pltpu.CompilerParams(vmem_limit_bytes=67043328),
        cost_estimate=pl.CostEstimate(flops=flops, bytes_accessed=1 << 20, transcendentals=0),
    )(*operands)


def swapped_pairs(size, offset):
    route = []
    for i in range(offset, size + offset, 2):
        one, two = i % size, (i + 1) % size
        route += [(one, two), (two, one)]
    return route


def exchange(outer, inner, sub):
    size = lax.axis_size("dom")
    outer = lax.ppermute(outer, "dom", swapped_pairs(size, 1))
    inner = lax.ppermute(inner, "dom", swapped_pairs(size, 0))
    group = lax.all_to_all(sub, "sub", 0, 0, tiled=True)
    return group, outer, inner


def shards(state, geometry, face_scale, material, cluster, neighbours, orientation,
           stiffness, jacobians, flux_local, flux_neigh, flux_plus, flux_minus):
    material = material.reshape(1, E)
    cluster = cluster.reshape(1, E)
    cube = arr(V, B, E)
    square = arr(V * V, E)
    packed = [arr(ROWS, E), arr(ROWS, COPY), arr(ROWS, COPY), arr(8, 48, 128)]
    wide = (112, V * E)
    narrow = (48, V * E)
    picked = (ROWS, 4 * E)
    jac, stiff, flocal, fneigh, fplus, fminus = [
        jnp.transpose(x, order)
        for x, order in [(jacobians, (0, 2, 1, 3))]
        + [(x, (1, 0, 2)) for x in (stiffness, flux_local, flux_neigh, flux_plus, flux_minus)]
    ]

    ejac, p, outer, inner, sub = call(
        first_kernel, [arr(27 * V, E), *packed], [(48, B), narrow, (V, V, V)],
        1 << 28, jac, material, geometry, stiff, state,
    )
    group, outer, inner = exchange(outer, inner, sub)
    local, plus, minus, turn, matrix = call(
        local_kernel_one,
        [cube, square, square, arr(4 * B, B, E), arr(112, B)],
        [wide, picked, (3, V, V), (3, V, V), (12, B, B), (48, B)], 1 << 33,
        fneigh, orientation, face_scale, fplus, fminus, material, stiff, flocal,
        neighbours, p, ejac,
    )
    base, p, outer, inner, sub = call(
        middle_kernel, [cube, *packed], [picked, (48, B), narrow, (V, B, E)],
        1 << 28, neighbours, outer, inner, group, turn, minus,
        state, local, cluster, ejac, stiff,
    )
    group, outer, inner = exchange(outer, inner, sub)
    local, = call(
        local_kernel_two, [cube], [wide, picked], 1 << 33,
        p, matrix, neighbours, ejac, face_scale, plus, turn, minus,
    )
    return call(
        last_kernel, [cube], [picked], 1 << 28,
        neighbours, outer, inner, group, turn, minus, base, local,
    )[0]


def solution(mesh):
    whole = ("dom", "sub")
    placed = (
        P(None, None, whole), P(None, None, whole), P(None, whole), P(whole), P(whole),
        P(None, whole), P(None, whole), P(), P(), P(), P(), P(), P(),
    )
    return jax.shard_map(
        shards, mesh=mesh, in_specs=placed, out_specs=P(None, None, whole), check_vma=False
    )
```
